1024 devices in a mesh: replica: 64 (over z, x_hi, core), tp: 16 (over x_lo, y).
Axes of the slice: x: 8 (x_hi: 4, x_lo: 2; x = x_hi * 2 + x_lo), y: 8, z: 8, core: 2. Of those that a mesh axis runs over, the one named last changes fastest.
Arguments:
- token_ids: int32 [1024], replicated, may hold values from 0 to 65535
- embed_table: bfloat16 [65536, 8192], P('replica', 'tp'), may hold values from -6 to 6
- norm_gain: bfloat16 [8192], replicated, may hold values from 0.099609375 to 1.8984375
- w_query: bfloat16 [8192, 4096], P(('replica', 'tp')), may hold values from -0.0625 to 0.0625
- w_keyvalue: bfloat16 [8192, 2, 512], P(('replica', 'tp')), may hold values from -0.0625 to 0.0625
- key_cache: bfloat16 [4096, 1024, 128], P(('replica', 'tp')), may hold values from -360 to 360
- value_cache: bfloat16 [4096, 1024, 128], P(('replica', 'tp')), may hold values from -6 to 6
- cache_lengths: int32 [1024], P('replica'), may hold values from 1 to 1024, as said below
Outputs:
- context: bfloat16 [4096, 1024], P(('replica', 'tp'))
- query_weight_tp: bfloat16 [8192, 4096], P(None, 'tp')
- keyvalue_weight_tp: bfloat16 [8192, 2, 512], P(None, None, 'tp')
The draws below stay inside these ranges and needn't reach their ends.
Inputs may be any that keep to these rules, and one draw needn't show every extreme that they name: `cache_lengths`: some sequence has exactly 1024 filled slots.
All inputs are finite; a program needn't handle non-finite values.
Results may differ from the reference program's by a relative error of at most 0.019.
The reference program's roundings to bfloat16 on the way count: a program that leaves them out, or rounds other values in their place, can miss the bound.
Values may be sent and summed in bfloat16 or wider, within the bound.
A program may use at most 64 MiB of HBM per device.

```python
import math
import jax
import jax.numpy as jnp
import numpy as np
from jax import lax

D = 8192
HD = 128
QHEADS = 32
KVHEADS = 4
BATCH = 16
CTX = 1024
VOCAB = 65536
GROUP = 8
SEQS = 1024
CACHE_ROWS = 4096
N_REPLICA = 64


def draw_key_cache(key, part):
    base = jnp.clip(jax.random.normal(key, (CACHE_ROWS, CTX, HD), jnp.float32), -6.0, 6.0)
    return base.astype(jnp.bfloat16)


def draw_cache_lengths(key, part):
    lengths = jax.random.randint(key, (SEQS,), 1, CTX + 1, jnp.int32)
    chosen = jax.random.randint(jax.random.fold_in(key, 3), (), 0, SEQS, jnp.int32)
    return jnp.where(jnp.arange(SEQS, dtype=jnp.int32) == chosen, CTX, lengths).astype(jnp.int32)


def plant(array, key, low, high):
    dims = array.shape
    spot = [jax.random.randint(jax.random.fold_in(key, axis), (), 0, dims[axis]) for axis in range(len(dims))]
    array = array.at[tuple(spot)].set(low)
    longest = dims.index(max(dims))
    spot[longest] = (spot[longest] + 1) % dims[longest]
    return array.at[tuple(spot)].set(high)


def level_of(stream_key, extent, pieces, least, largest):
    level = 1.0
    for dim, shards_of in pieces:
        heights = jax.random.uniform(jax.random.fold_in(jax.random.fold_in(stream_key, 6), dim), (shards_of,), jnp.float32, least / len(pieces), largest / len(pieces))
        level = level * jnp.repeat(jnp.exp(heights), extent[dim] // shards_of).reshape((-1,) + (1,) * (len(extent) - 1 - dim))
    return level


def rank_bounds(amount, skew):
    weights = [(1 << 20) // math.isqrt(grade ** skew) + 1 for grade in range(1, amount + 1)]
    spread = 1 + sum(weights) // (1 << 30)
    return np.cumsum(np.array([max(1, weight // spread) for weight in weights]))


def ranked(key, dims, number_of, skew):
    listing = rank_bounds(number_of, skew)
    ticket = jax.random.randint(jax.random.fold_in(key, 1), dims, 0, int(listing[number_of - 1]))
    grade = jnp.searchsorted(jnp.asarray(listing, jnp.int32), ticket, side="right")
    return jax.random.permutation(jax.random.fold_in(key, 2), number_of)[grade].astype(jnp.int32)


def normal_values(own_key, extent, width, limit, shards=(), held_as=jnp.bfloat16):
    gain = level_of(own_key, extent, shards, -0.22, 0.18) if shards else 1.0
    array = jax.random.normal(own_key, extent, jnp.float32) * width * gain
    return jnp.minimum(jnp.maximum(array, -limit), limit).astype(held_as)


def setup_inputs(seed: int = 0) -> dict:
    arg_keys = jax.random.split(jax.random.key(seed), 9)
    return {
        "token_ids": plant(ranked(arg_keys[0], (SEQS,), VOCAB, 2), jax.random.fold_in(arg_keys[0], 3), 0, VOCAB - 1).astype(jnp.int32),
        "embed_table": normal_values(arg_keys[1], (VOCAB, D), 1.0, 6.0, ((0, 64), (1, 16))),
        "norm_gain": jnp.clip(1.0 + 0.18 * jax.random.normal(arg_keys[2], (D,), jnp.float32), 0.099609375, 1.8984375).astype(jnp.bfloat16),
        "w_query": normal_values(arg_keys[3], (D, QHEADS * HD), D ** -0.5, 0.0625, ((0, 1024),)),
        "w_keyvalue": normal_values(arg_keys[4], (D, 2, KVHEADS * HD), D ** -0.5, 0.0625, ((0, 1024),)),
        "key_cache": draw_key_cache(jax.random.fold_in(arg_keys[8], 71), 0),
        "value_cache": normal_values(arg_keys[6], (CACHE_ROWS, CTX, HD), 1.0, 6.0, ((0, 1024),)),
        "cache_lengths": draw_cache_lengths(jax.random.fold_in(arg_keys[8], 71), 0),
    }


def attend(query, keys, values, key_new, value_new, lengths):
    scale = query.shape[-1] ** (-0.5)
    scores = jnp.einsum('rgd,rcd->rgc', query.astype(jnp.float32), keys.astype(jnp.float32)) * scale
    position = lax.broadcasted_iota(jnp.int32, scores.shape, 2)
    scores = jnp.where(position < lengths[:, None, None], scores, -jnp.inf)
    own = jnp.einsum('rgd,rd->rg', query.astype(jnp.float32), key_new.astype(jnp.float32)) * scale
    top = jnp.maximum(lax.optimization_barrier(jnp.max(scores, axis=2)), own)
    weights = jnp.exp(scores - top[:, :, None])
    own_weight = jnp.exp(own - top)
    total = lax.optimization_barrier(jnp.sum(weights, axis=2)) + own_weight
    weights = (weights / total[:, :, None]).astype(jnp.bfloat16)
    own_weight = (own_weight / total).astype(jnp.bfloat16)
    context = jnp.einsum('rgc,rcd->rgd', weights.astype(jnp.float32), values.astype(jnp.float32))
    context = context + own_weight.astype(jnp.float32)[:, :, None] * value_new.astype(jnp.float32)[:, None, :]
    return context.astype(jnp.bfloat16)

def reference(token_ids, embed_table, norm_gain, w_query, w_keyvalue, key_cache, value_cache, cache_lengths):
    query_weight_tp = w_query
    keyvalue_weight_tp = w_keyvalue
    embedded = jnp.take(embed_table, token_ids, axis=0)
    values32 = embedded.astype(jnp.float32)
    mean_square = lax.optimization_barrier(jnp.mean(values32 * values32, axis=1, keepdims=True))
    normed = (values32 * lax.rsqrt(mean_square + 1e-05) * norm_gain.astype(jnp.float32)).astype(jnp.bfloat16)
    query = jnp.dot(normed, w_query, preferred_element_type=jnp.float32).astype(jnp.bfloat16)
    pair = jnp.dot(normed, w_keyvalue.reshape(D, 2 * KVHEADS * HD), preferred_element_type=jnp.float32).astype(jnp.bfloat16)
    pair = pair.reshape(SEQS, 2, KVHEADS * HD)
    query = query.reshape(N_REPLICA, BATCH, KVHEADS, GROUP, HD).transpose(0, 2, 1, 3, 4).reshape(N_REPLICA, KVHEADS * BATCH, GROUP, HD)
    key_new = pair[:, 0].reshape(N_REPLICA, BATCH, KVHEADS, HD).transpose(0, 2, 1, 3).reshape(N_REPLICA, KVHEADS * BATCH, HD)
    value_new = pair[:, 1].reshape(N_REPLICA, BATCH, KVHEADS, HD).transpose(0, 2, 1, 3).reshape(N_REPLICA, KVHEADS * BATCH, HD)
    keys = key_cache.reshape(N_REPLICA, KVHEADS * BATCH, CTX, HD)
    values = value_cache.reshape(N_REPLICA, KVHEADS * BATCH, CTX, HD)
    lengths = jnp.tile(cache_lengths.reshape(N_REPLICA, BATCH), (1, KVHEADS))

    def per_group(items):
        return attend(items[0], items[1], items[2], items[3], items[4], items[5])
    context = lax.map(per_group, (query, keys, values, key_new, value_new, lengths))
    context = context.reshape(CACHE_ROWS, GROUP * HD)
    return (context, query_weight_tp, keyvalue_weight_tp)
```

```python
import functools
import jax
import jax.numpy as jnp
from jax import lax
from jax.experimental import pallas as pl
from jax.experimental.pallas import tpu as pltpu
from jax.sharding import PartitionSpec as P

MESH = pl.DeviceIdType.MESH
Z, XH, CORES, TPS = 8, 4, 2, 16
GROUPS = Z * XH * CORES
BATCH, HEAD, GROUP, KVH = 16, 128, 8, 4
FEAT = 512
ROWS = 128
BLOCK = 160
HALF = BLOCK // 2
QCOLS = 256
KVCOLS = 64
MSG = 384


def ring_events(block_us=1.76, lag_us=2.2, first_us=(0.0, 4.5, 9.0, 4.5)):
    ready = [(first_us[j], 0, j) for j in range(XH)]
    free, events = 0.0, []
    while ready:
        ready.sort()
        at, step, j = ready.pop(0)
        if step == 0:
            events.append((at, 0, j))
        else:
            events.append((at, step, j))
        if step < 4:
            begin = max(free, at)
            free = begin + (block_us if step < 3 else block_us / 2)
            ready.append((free + lag_us, step + 1, j))
    return events


def handoff_kernel(
    msg, part, gain, blocks, mixed,
    pieces, got_core, sums_core, got_x, sums_x, got_z, sums_z, embedded, normed, sent, acc_q, acc_kv,
    p1_s, p1_r, xw_s, xw_r, zp_s, zp_r, zm_s, zm_r, pf_s, pf_r, e1_s, e1_r, e2_s, e2_r, e3_s, e3_r,
    e4_s, e4_r, e7_s, e7_r,
):
    r, t = lax.axis_index("replica"), lax.axis_index("tp")
    z, xh, c = r // 8, (r // 2) % 4, r % 2

    def rep(z_, xh_, c_):
        return (z_ * XH + xh_) * CORES + c_

    def dev(rep_, tp_):
        return {"replica": rep_, "tp": tp_}

    partner = dev(rep(z, xh, 1 - c), t)

    def x_peer(d):
        return dev(rep(z, (xh + d) % XH, c), t)

    def z_peer(d):
        return dev(rep((z + d) % Z, xh, c), t)

    def t_peer(d):
        return dev(r, (t + d) % TPS)

    barrier = pltpu.get_barrier_semaphore()
    peers = [partner] + [x_peer(d) for d in (1, 2, 3)] + [z_peer(d) for d in range(1, 8)]
    peers += [t_peer(d) for d in range(1, 16)]
    for p in peers:
        pl.semaphore_signal(barrier, inc=1, device_id=p, device_id_type=MESH)

    started = []

    def send(src, dst, ss, rs, to):
        copy = pltpu.make_async_remote_copy(
            src_ref=src, dst_ref=dst, send_sem=ss, recv_sem=rs, device_id=to, device_id_type=MESH
        )
        copy.start()
        started.append(copy)

    def arrived(dst, rs, frm):
        pltpu.make_async_remote_copy(
            src_ref=dst, dst_ref=dst, send_sem=rs, recv_sem=rs, device_id=frm, device_id_type=MESH
        ).wait_recv()

    pieces[t] = msg[t]
    pl.semaphore_wait(barrier, len(peers))

    send(part.at[1 - c], got_core, e1_s.at[0], e1_r.at[0], partner)
    for d in range(1, 16):
        send(msg.at[(t + d) % TPS], pieces.at[t], p1_s.at[d], p1_r.at[d], t_peer(d))

    arrived(got_core, e1_r.at[0], partner)

    @pl.loop(0, XH)
    def _(a):
        sums_core[a] = part[c, a] + got_core[a]

    for d in range(1, 16):
        arrived(pieces.at[(t - d + TPS) % TPS], p1_r.at[d], t_peer(d))
    own = rep(z, xh, c)
    blocks[own, 0:ROWS, :] = pieces[:, :, 0:QCOLS].reshape(ROWS, QCOLS)
    turned = pieces[:, :, QCOLS:MSG].reshape(ROWS, HEAD).astype(jnp.float32).T.astype(jnp.bfloat16)
    blocks[own, ROWS:BLOCK, 0:HEAD] = turned[0:32]
    blocks[own, ROWS:BLOCK, HEAD:QCOLS] = turned[32:64]

    def block_id(dz, j):
        return rep((z + dz + 2 * Z) % Z, (xh - j + XH) % XH, c)

    def mirrored(dz, j):
        return rep((z + dz + 2 * Z) % Z, (xh - j + XH) % XH, 1 - c)

    lower, upper = pl.ds(0, HALF), pl.ds(HALF, HALF)

    def to_ring(j, step):
        up, down = blocks.at[block_id(-step, j)], blocks.at[block_id(step, j)]
        if step == 3:
            up, down = up.at[lower], down.at[upper]
        send(up, up, zp_s.at[j, step], zp_r.at[j, step], z_peer(1))
        send(down, down, zm_s.at[j, step], zm_r.at[j, step], z_peer(Z - 1))

    def to_partner(ref, k, j):
        send(ref, ref, pf_s.at[j, k], pf_r.at[j, k], partner)

    def on_block(step, j):
        if step == 0:
            if j:
                arrived(blocks.at[block_id(0, j)], xw_r.at[j], x_peer(XH - j))
            to_ring(j, 0)
            if j == 0:
                for d in (1, 3, 2):
                    send(blocks.at[own], blocks.at[own], xw_s.at[d], xw_r.at[d], x_peer(d))
            to_partner(blocks.at[block_id(0, j)], 0, j)
            return
        up, down = blocks.at[block_id(-step, j)], blocks.at[block_id(step, j)]
        if step == 4:
            up, down = up.at[lower], down.at[upper]
        arrived(up, zp_r.at[j, step - 1], z_peer(Z - 1))
        arrived(down, zm_r.at[j, step - 1], z_peer(1))
        if step < 4:
            to_ring(j, step)
        to_partner(up, 2 * step - 1, j)
        to_partner(down, 2 * step, j)

    def send_x_sums():
        for d in (1, 3, 2):
            send(sums_core.at[(xh + d) % XH], got_x.at[d - 1], e2_s.at[d], e2_r.at[d], x_peer(d))

    def add_x_sums():
        for d in (1, 3, 2):
            arrived(got_x.at[d - 1], e2_r.at[d], x_peer(XH - d))

        @pl.loop(0, Z)
        def _(a):
            sums_x[a] = (sums_core[xh, a] + got_x[0, a]) + (got_x[1, a] + got_x[2, a])

        for d in (4, 3, 5, 2, 6, 1, 7):
            send(sums_x.at[(z + d) % Z], got_z.at[d - 1], e3_s.at[d], e3_r.at[d], z_peer(d))

    def add_z_sums():
        for d in range(1, 8):
            arrived(got_z.at[d - 1], e3_r.at[d], z_peer(Z - d))
        total = sums_x[z]
        for d in range(1, 8):
            total = total + got_z[d - 1]
        sums_z[...] = total
        embedded[t] = total
        for d in (12, 4, 11, 5, 13, 3, 10, 6, 14, 2, 9, 7, 15, 1, 8):
            send(sums_z, embedded.at[t], e4_s.at[d], e4_r.at[d], t_peer(d))

    todo = [(at, 0, functools.partial(on_block, step, j)) for at, step, j in ring_events()]
    todo += [(0.1, 1, send_x_sums), (18.0, 1, add_x_sums), (24.0, 1, add_z_sums)]
    for _, _, act in sorted(todo, key=lambda item: item[:2]):
        act()

    for d in range(1, 16):
        arrived(embedded.at[(t - d + TPS) % TPS], e4_r.at[d], t_peer(d))

    def squares(k, total):
        v = embedded[k].astype(jnp.float32)
        return total + v * v

    squared = lax.fori_loop(0, TPS, squares, jnp.zeros((BATCH, FEAT), jnp.float32))
    mean_square = jnp.sum(squared, axis=1, keepdims=True) * (1.0 / (TPS * FEAT))
    factor = lax.rsqrt(mean_square + 1e-05)

    @pl.loop(0, TPS)
    def _(k):
        normed[k] = (embedded[k].astype(jnp.float32) * factor * gain[k].astype(jnp.float32)).astype(
            jnp.bfloat16
        )

    for j in range(XH):
        arrived(blocks.at[mirrored(0, j)], pf_r.at[j, 0], partner)
        for step in range(1, 5):
            up, down = blocks.at[mirrored(-step, j)], blocks.at[mirrored(step, j)]
            if step == 4:
                up, down = up.at[lower], down.at[upper]
            arrived(up, pf_r.at[j, 2 * step - 1], partner)
            arrived(down, pf_r.at[j, 2 * step], partner)

    acc_q[...] = jnp.zeros_like(acc_q)
    acc_kv[...] = jnp.zeros_like(acc_kv)

    @pl.loop(0, TPS)
    def _(k):
        lhs = normed[k]
        rows = [blocks[4 * k + i, 0:ROWS, :] for i in range(4)]
        acc_q[...] += jnp.dot(
            lhs, jnp.concatenate(rows, axis=0), preferred_element_type=jnp.float32
        )
        keys = [blocks[4 * k + i, ROWS:BLOCK, 0:HEAD] for i in range(4)]
        values = [blocks[4 * k + i, ROWS:BLOCK, HEAD:QCOLS] for i in range(4)]
        both = jnp.concatenate(
            [jnp.concatenate(keys, axis=1), jnp.concatenate(values, axis=1)], axis=0
        )
        acc_kv[:, 0:KVCOLS] += lax.dot_general(
            lhs, both, (((1,), (1,)), ((), ())), preferred_element_type=jnp.float32
        )

    quarter = t % 4
    for i in range(4):
        sent[i, :, 0:QCOLS] = acc_q[4 * i : 4 * i + 4, :].astype(jnp.bfloat16)
        sent[i, :, QCOLS:MSG] = acc_kv[4 * i : 4 * i + 4, :].astype(jnp.bfloat16)
    mixed[quarter] = sent[quarter]
    for d in range(1, 4):
        to = (quarter + d) % 4
        send(sent.at[to], mixed.at[quarter], e7_s.at[d], e7_r.at[d], dev(r, t - quarter + to))
    for d in range(1, 4):
        frm = (quarter - d + 4) % 4
        arrived(mixed.at[frm], e7_r.at[d], dev(r, t - quarter + frm))
    for copy in started:
        copy.wait_send()


def handoff(msg, part, gain):
    bf16, f32 = jnp.bfloat16, jnp.float32
    vmem = pl.BlockSpec(memory_space=pltpu.VMEM)
    dma = pltpu.SemaphoreType.DMA
    return pl.pallas_call(
        handoff_kernel,
        out_shape=(
            jax.ShapeDtypeStruct((GROUPS, BLOCK, QCOLS), bf16),
            jax.ShapeDtypeStruct((4, 4, MSG), bf16),
        ),
        in_specs=[vmem] * 3,
        out_specs=(vmem, vmem),
        scratch_shapes=[
            pltpu.VMEM((TPS, 8, MSG), bf16),
            pltpu.VMEM((XH, Z, BATCH, FEAT), bf16),
            pltpu.VMEM((XH, Z, BATCH, FEAT), bf16),
            pltpu.VMEM((3, Z, BATCH, FEAT), bf16),
            pltpu.VMEM((Z, BATCH, FEAT), bf16),
            pltpu.VMEM((7, BATCH, FEAT), bf16),
            pltpu.VMEM((BATCH, FEAT), bf16),
            pltpu.VMEM((TPS, BATCH, FEAT), bf16),
            pltpu.VMEM((TPS, BATCH, FEAT), bf16),
            pltpu.VMEM((4, 4, MSG), bf16),
            pltpu.VMEM((BATCH, QCOLS), f32),
            pltpu.VMEM((BATCH, HEAD), f32),
            dma((16,)), dma((16,)), dma((4,)), dma((4,)),
            dma((4, 4)), dma((4, 4)), dma((4, 4)), dma((4, 4)),
            dma((4, 9)), dma((4, 9)), dma((1,)), dma((1,)),
            dma((4,)), dma((4,)), dma((8,)), dma((8,)),
            dma((16,)), dma((16,)), dma((4,)), dma((4,)),
        ],
        compiler_params=pltpu.CompilerParams(
            collective_id=0, has_side_effects=True, vmem_limit_bytes=40 << 20
        ),
        cost_estimate=pl.CostEstimate(flops=1 << 34, bytes_accessed=1 << 23, transcendentals=0),
        name="handoff",
    )(msg, part, gain)


def attend_kernel(
    lengths, mixed, blocks, keys_hbm, values_hbm, context, query_out, pair_out, keys, values, pair, sems
):
    copies = [
        pltpu.make_async_copy(keys_hbm, keys, sems.at[0]),
        pltpu.make_async_copy(values_hbm, values, sems.at[1]),
        pltpu.make_async_copy(blocks.at[:, 0:ROWS, :], query_out, sems.at[2]),
    ]
    for copy in copies:
        copy.start()

    for g in range(GROUPS):
        pair[0:32, g * ROWS : (g + 1) * ROWS] = blocks[g, ROWS:BLOCK, 0:HEAD]
        pair[32:64, g * ROWS : (g + 1) * ROWS] = blocks[g, ROWS:BLOCK, HEAD:QCOLS]
    last = pltpu.make_async_copy(pair, pair_out, sems.at[3])
    last.start()
    got = [mixed[j].astype(jnp.float32) for j in range(4)]
    scale = HEAD ** (-0.5)
    copies[0].wait()
    rows = []
    for r in range(4):
        heads = [got[j][r : r + 1, k * HEAD : (k + 1) * HEAD] for j in range(4) for k in range(2)]
        query32 = jnp.concatenate(heads, axis=0)
        query = query32.astype(jnp.bfloat16)
        key_new = jnp.concatenate([got[j][r : r + 1, QCOLS : QCOLS + 32] for j in range(4)], axis=1)
        value_new = jnp.concatenate(
            [got[j][r : r + 1, QCOLS + 32 : QCOLS + 64] for j in range(4)], axis=1
        )
        scores = (
            lax.dot_general(
                query, keys[r], (((1,), (1,)), ((), ())), preferred_element_type=jnp.float32
            )
            * scale
        )
        position = lax.broadcasted_iota(jnp.int32, scores.shape, 1)
        scores = jnp.where(position < lengths[r], scores, -jnp.inf)
        own = jnp.sum(query32 * key_new, axis=1, keepdims=True) * scale
        top = jnp.maximum(jnp.max(scores, axis=1, keepdims=True), own)
        weights = jnp.exp(scores - top)
        own_weight = jnp.exp(own - top)
        total = jnp.sum(weights, axis=1, keepdims=True) + own_weight
        weights = (weights / total).astype(jnp.bfloat16)
        own_weight = (own_weight / total).astype(jnp.bfloat16).astype(jnp.float32)
        if r == 0:
            copies[1].wait()
        found = jnp.dot(weights, values[r], preferred_element_type=jnp.float32)
        rows.append(found + own_weight * value_new)
    lanes = [jnp.concatenate([rows[r][h : h + 1] for r in range(4)], axis=0) for h in range(GROUP)]
    context[...] = jnp.concatenate(lanes, axis=1).astype(jnp.bfloat16)
    copies[2].wait()
    last.wait()


def attend(lengths, mixed, blocks, keys, values):
    bf16 = jnp.bfloat16
    vmem = pl.BlockSpec(memory_space=pltpu.VMEM)
    anywhere = pl.BlockSpec(memory_space=pl.ANY)
    hbm = pl.BlockSpec(memory_space=pltpu.HBM)
    return pl.pallas_call(
        attend_kernel,
        out_shape=(
            jax.ShapeDtypeStruct((4, GROUP * HEAD), bf16),
            jax.ShapeDtypeStruct((GROUPS, ROWS, QCOLS), bf16),
            jax.ShapeDtypeStruct((KVCOLS, GROUPS * ROWS), bf16),
        ),
        in_specs=[pl.BlockSpec(memory_space=pltpu.SMEM), vmem, vmem, anywhere, anywhere],
        out_specs=(vmem, hbm, hbm),
        scratch_shapes=[
            pltpu.VMEM((4, 1024, HEAD), bf16),
            pltpu.VMEM((4, 1024, HEAD), bf16),
            pltpu.VMEM((KVCOLS, GROUPS * ROWS), bf16),
            pltpu.SemaphoreType.DMA((4,)),
        ],
        compiler_params=pltpu.CompilerParams(vmem_limit_bytes=24 << 20),
        name="attend",
    )(lengths, mixed, blocks, keys, values)


def per_device(
    token_ids, embed_table, norm_gain, w_query, w_keyvalue, key_cache, value_cache, cache_lengths
):
    r, t = lax.axis_index("replica"), lax.axis_index("tp")
    vocab_rows = embed_table.shape[0]
    ids = token_ids.reshape(Z, XH, CORES, BATCH).transpose(2, 1, 0, 3).reshape(-1)
    columns = lax.broadcasted_iota(jnp.int32, (ids.shape[0], vocab_rows), 1)
    onehot = ((ids - r * vocab_rows)[:, None] == columns).astype(jnp.bfloat16)
    part = jnp.dot(onehot, embed_table, preferred_element_type=jnp.float32).astype(jnp.bfloat16)
    part = part.reshape(CORES, XH, Z, BATCH, FEAT)
    query_cols = w_query.reshape(8, TPS, QCOLS).transpose(1, 0, 2)
    pair_cols = w_keyvalue.reshape(8, 2, TPS, 32).transpose(2, 0, 1, 3).reshape(TPS, 8, KVCOLS)
    filler = jnp.zeros((TPS, 8, MSG - QCOLS - KVCOLS), jnp.bfloat16)
    msg = jnp.concatenate([query_cols, pair_cols, filler], axis=2)
    blocks, mixed = handoff(msg, part, norm_gain.reshape(TPS, 1, FEAT))
    lengths = lax.dynamic_slice_in_dim(cache_lengths, (t % 4) * 4, 4, 0)
    context, query_full, pair_full = attend(lengths, mixed, blocks, key_cache, value_cache)
    return (
        context,
        query_full.reshape(GROUPS * ROWS, QCOLS),
        pair_full.reshape(2, 32, GROUPS * ROWS).transpose(2, 0, 1),
    )


def solution(mesh):
    both = ("replica", "tp")
    placed = (
        P(),
        P("replica", "tp"),
        P(),
        P(both, None),
        P(both, None, None),
        P(both, None, None),
        P(both, None, None),
        P("replica"),
    )
    return jax.shard_map(
        per_device,
        mesh=mesh,
        in_specs=placed,
        out_specs=(P(both, None), P(None, "tp"), P(None, None, "tp")),
        check_vma=False,
    )
```

```python
import functools
import jax
import jax.numpy as jnp
from jax import lax
from jax.experimental import pallas as pl
from jax.experimental.pallas import tpu as pltpu
from jax.sharding import PartitionSpec as P

MESH = pl.DeviceIdType.MESH
Z, XH, CORES, TPS = 8, 4, 2, 16
GROUPS = Z * XH * CORES
BATCH, HEAD, GROUP, KVH = 16, 128, 8, 4
FEAT = 512
ROWS = 128
BLOCK = 160
QCOLS = 256
KVCOLS = 64
MSG = 384
PIECES = 2
PIECE = BLOCK // PIECES


def link_events():
    lag, block, token = 2.2, 1.76 / PIECES, 1.4
    ready = [(1.5, "sum", 0)]
    for j, at in ((0, 6.5), (1, 10.5), (3, 10.5), (2, 13.5)):
        ready += [(at + 1.7 * p, "block", j, p, 0) for p in range(PIECES)]
    free, events = 0.0, []
    while ready:
        ready.sort()
        at, kind, *what = ready.pop(0)
        events.append((at, kind, *what))
        if what[-1] == 4:
            continue
        if kind == "sum":
            took = token / 2 if what[-1] == 0 else token
        else:
            took = block / 2 if what[-1] == 3 else block
        free = max(free, at) + took
        ready.append((free + lag, kind, *what[:-1], what[-1] + 1))
    return events


def handoff_kernel(
    ids, gain, table_hbm, query_hbm, pair_hbm, blocks, pair, mixed,
    table, query, pairs, part, got_core, sums, up_sums, down_sums, got_x, sum_x, own_pairs, turned, embedded,
    normed, sent, acc_q, acc_kv,
    in_s, p1_s, p1_r, p2_s, p2_r, xw_s, xw_r, zp_s, zp_r, zm_s, zm_r, pf_s, pf_r, e1_s, e1_r, eu_s, eu_r, ed_s, ed_r,
    e2_s, e2_r, e4_s, e4_r, e7_s, e7_r,
):
    r, t = lax.axis_index("replica"), lax.axis_index("tp")
    z, xh, c = r // 8, (r // 2) % 4, r % 2
    f32, bf16 = jnp.float32, jnp.bfloat16

    def rep(z_, xh_, c_):
        return (z_ * XH + xh_) * CORES + c_

    def dev(rep_, tp_):
        return {"replica": rep_, "tp": tp_}

    partner = dev(rep(z, xh, 1 - c), t)

    def x_peer(d):
        return dev(rep(z, (xh + d) % XH, c), t)

    def z_peer(d):
        return dev(rep((z + d) % Z, xh, c), t)

    def t_peer(d):
        return dev(r, (t + d) % TPS)

    loads = [
        pltpu.make_async_copy(table_hbm, table, in_s.at[0]),
        pltpu.make_async_copy(query_hbm, query, in_s.at[1]),
        pltpu.make_async_copy(pair_hbm, pairs, in_s.at[2]),
    ]
    for load in loads:
        load.start()
    barrier = pltpu.get_barrier_semaphore()
    peers = [partner] + [x_peer(d) for d in (1, 2, 3)] + [z_peer(1), z_peer(Z - 1)]
    peers += [t_peer(d) for d in range(1, 16)]
    for p in peers:
        pl.semaphore_signal(barrier, inc=1, device_id=p, device_id_type=MESH)

    started = []

    def send(src, dst, ss, rs, to):
        copy = pltpu.make_async_remote_copy(
            src_ref=src, dst_ref=dst, send_sem=ss, recv_sem=rs, device_id=to, device_id_type=MESH
        )
        copy.start()
        started.append(copy)

    def arrived(dst, rs, frm):
        pltpu.make_async_remote_copy(
            src_ref=dst, dst_ref=dst, send_sem=rs, recv_sem=rs, device_id=frm, device_id_type=MESH
        ).wait_recv()

    base = r * table.shape[0]
    loads[0].wait()
    lane = lax.broadcasted_iota(jnp.int32, (128, 128), 1)

    @pl.loop(0, Z)
    def _(k):
        named = jnp.broadcast_to((ids[pl.ds(k, 1), :] - base).astype(f32), (128, 128)).T
        hot = jnp.concatenate(
            [(named == (lane + 128 * q).astype(f32)).astype(bf16) for q in range(8)], axis=1
        )
        rows = jnp.dot(hot, table[...], preferred_element_type=f32).astype(bf16)
        rows = rows.reshape(XH, CORES, BATCH, FEAT)
        part[0, k] = rows[:, 0]
        part[1, k] = rows[:, 1]

    own = rep(z, xh, c)
    first_row = pl.multiple_of(t * 8, 8)
    heads_at = pl.multiple_of((t // 4) * 128, 128)
    loads[1].wait()
    loads[2].wait()
    blocks[own, pl.ds(first_row, 8), :] = query[:, pl.ds(pl.multiple_of(t * QCOLS, QCOLS), QCOLS)]
    own_pairs[t] = pairs[:, :, pl.ds(heads_at, 128)]
    pl.semaphore_wait(barrier, len(peers))

    def turn_z(d):
        return (z + d) % Z

    core_order = (4, 3, 5, 2, 6, 1, 7, 0)
    for d in core_order:
        send(part.at[1 - c, turn_z(d)], got_core.at[turn_z(d)], e1_s.at[d], e1_r.at[d], partner)
    for d in (12, 4, 11, 5, 13, 3, 10, 6, 14, 2, 9, 7, 15, 1, 8):
        to = (t + d) % TPS
        send(
            query.at[:, pl.ds(pl.multiple_of(to * QCOLS, QCOLS), QCOLS)],
            blocks.at[own, pl.ds(first_row, 8), :],
            p1_s.at[d], p1_r.at[d], t_peer(d),
        )
        send(
            pairs.at[:, :, pl.ds(pl.multiple_of((to // 4) * 128, 128), 128)],
            own_pairs.at[t],
            p2_s.at[d], p2_r.at[d], t_peer(d),
        )

    def add_core(d):
        arrived(got_core.at[turn_z(d)], e1_r.at[d], partner)
        sums[turn_z(d)] = part[c, turn_z(d)] + got_core[turn_z(d)]

    def on_sum(step):
        up_dst, down_dst = up_sums.at[step], down_sums.at[step]
        if step == 0:
            add_core(4)
            up, down = sums.at[turn_z(4), pl.ds(0, 2)], sums.at[turn_z(4), pl.ds(2, 2)]
            up_dst, down_dst = up_dst.at[pl.ds(0, 2)], down_dst.at[pl.ds(2, 2)]
        else:
            up, down = up_sums.at[step - 1], down_sums.at[step - 1]
            up_got, down_got = up, down
            if step == 1:
                up_got, down_got = up.at[pl.ds(0, 2)], down.at[pl.ds(2, 2)]
            arrived(up_got, eu_r.at[step - 1], z_peer(Z - 1))
            arrived(down_got, ed_r.at[step - 1], z_peer(1))
            if step == 4:
                add_z()
                return
            above, below = turn_z(4 - step), turn_z(4 + step)
            if step == 1:
                up_sums[0, 0:2] = up_sums[0, 0:2] + sums[above, 0:2]
                up_sums[0, 2:4] = sums[above, 2:4]
                down_sums[0, 2:4] = down_sums[0, 2:4] + sums[below, 2:4]
                down_sums[0, 0:2] = sums[below, 0:2]
            else:
                up_sums[step - 1] = up_sums[step - 1] + sums[above]
                down_sums[step - 1] = down_sums[step - 1] + sums[below]
        send(up, up_dst, eu_s.at[step], eu_r.at[step], z_peer(1))
        send(down, down_dst, ed_s.at[step], ed_r.at[step], z_peer(Z - 1))
        if step == 0:
            for d in core_order[1:]:
                add_core(d)

    def add_z():
        sum_x[...] = (sums[z] + up_sums[3]) + down_sums[3]
        for d in (2, 1, 3):
            send(sum_x.at[(xh + d) % XH], got_x.at[d - 1], e2_s.at[d], e2_r.at[d], x_peer(d))

    def add_x():
        for d in (1, 3, 2):
            arrived(got_x.at[d - 1], e2_r.at[d], x_peer(XH - d))
        embedded[t] = (sum_x[xh] + got_x[0]) + (got_x[1] + got_x[2])
        for d in (12, 4, 11, 5, 13, 3, 10, 6, 14, 2, 9, 7, 15, 1, 8):
            send(embedded.at[t], embedded.at[t], e4_s.at[d], e4_r.at[d], t_peer(d))

    def whole_block():
        for d in range(1, 16):
            frm = (t - d + TPS) % TPS
            arrived(own_pairs.at[frm], p2_r.at[d], t_peer(TPS - d))
        even = lax.broadcasted_iota(jnp.int32, (256, 256), 1)
        even = jnp.where(even < 128, 2 * even, 2 * even - 255)
        pick = (lax.broadcasted_iota(jnp.int32, (256, 256), 0) == even).astype(bf16)
        turned[...] = lax.dot_general(
            own_pairs[...].reshape(256, 128), pick, (((0,), (0,)), ((), ())),
            preferred_element_type=f32,
        )
        mine = pl.multiple_of((t % 4) * 32, 32)
        blocks[own, ROWS:BLOCK, :] = turned[pl.ds(mine, 32), :].astype(bf16)
        for d in range(1, 16):
            frm = (t - d + TPS) % TPS
            arrived(
                blocks.at[own, pl.ds(pl.multiple_of(frm * 8, 8), 8), :], p1_r.at[d], t_peer(TPS - d)
            )

    def block_id(dz, j):
        return rep((z + dz + 2 * Z) % Z, (xh - j + XH) % XH, c)

    def mirrored(dz, j):
        return rep((z + dz + 2 * Z) % Z, (xh - j + XH) % XH, 1 - c)

    def piece(ref, p):
        return ref.at[pl.ds(p * PIECE, PIECE)]

    def to_ring(j, p, step):
        up, down = piece(blocks.at[block_id(-step, j)], p), piece(blocks.at[block_id(step, j)], p)
        if step < 3 or p == 0:
            send(up, up, zp_s.at[j, p, step], zp_r.at[j, p, step], z_peer(1))
        if step < 3 or p == 1:
            send(down, down, zm_s.at[j, p, step], zm_r.at[j, p, step], z_peer(Z - 1))

    def to_partner(ref, k, j):
        send(ref, ref, pf_s.at[j, k], pf_r.at[j, k], partner)

    def on_block(j, p, step):
        if step == 0:
            if j == 0 and p == 0:
                whole_block()
            mine = piece(blocks.at[block_id(0, j)], p)
            if j:
                arrived(mine, xw_r.at[j, p], x_peer(XH - j))
            else:
                for d in (1, 3, 2):
                    send(mine, mine, xw_s.at[d, p], xw_r.at[d, p], x_peer(d))
            to_ring(j, p, 0)
            if p == PIECES - 1:
                to_partner(blocks.at[block_id(0, j)], 0, j)
            return
        up, down = blocks.at[block_id(-step, j)], blocks.at[block_id(step, j)]
        if step < 4 or p == 0:
            arrived(piece(up, p), zp_r.at[j, p, step - 1], z_peer(Z - 1))
        if step < 4 or p == 1:
            arrived(piece(down, p), zm_r.at[j, p, step - 1], z_peer(1))
        if step < 4:
            to_ring(j, p, step)
            if p == PIECES - 1:
                to_partner(up, 2 * step - 1, j)
                to_partner(down, 2 * step, j)
        else:
            to_partner(piece(up, p), 7 + p, j)

    def from_partner(step):
        for j in range(XH):
            up, down = blocks.at[mirrored(-step, j)], blocks.at[mirrored(step, j)]
            if step == 0:
                arrived(up, pf_r.at[j, 0], partner)
            elif step < 4:
                arrived(up, pf_r.at[j, 2 * step - 1], partner)
                arrived(down, pf_r.at[j, 2 * step], partner)
            else:
                for p in range(PIECES):
                    arrived(piece(up, p), pf_r.at[j, 7 + p], partner)

    def normalize():
        for d in range(1, 16):
            arrived(embedded.at[(t - d + TPS) % TPS], e4_r.at[d], t_peer(TPS - d))

        def squares(k, total):
            v = embedded[k].astype(f32)
            return total + v * v

        squared = lax.fori_loop(0, TPS, squares, jnp.zeros((BATCH, FEAT), f32))
        mean_square = jnp.sum(squared, axis=1, keepdims=True) * (1.0 / (TPS * FEAT))
        factor = lax.rsqrt(mean_square + 1e-05)

        @pl.loop(0, TPS)
        def _(k):
            normed[k] = (embedded[k].astype(f32) * factor * gain[k].astype(f32)).astype(bf16)

        acc_q[...] = jnp.zeros_like(acc_q)
        acc_kv[...] = jnp.zeros_like(acc_kv)

    def multiply(k):
        lhs = normed[k]
        rows = [blocks[4 * k + i, 0:ROWS, :] for i in range(4)]
        acc_q[...] += jnp.dot(lhs, jnp.concatenate(rows, axis=0), preferred_element_type=f32)
        keys = [blocks[4 * k + i, ROWS:BLOCK, 0:HEAD] for i in range(4)]
        values = [blocks[4 * k + i, ROWS:BLOCK, HEAD:QCOLS] for i in range(4)]
        both = jnp.concatenate(
            [jnp.concatenate(keys, axis=1), jnp.concatenate(values, axis=1)], axis=0
        )
        acc_kv[:, 0:KVCOLS] += lax.dot_general(
            lhs, both, (((1,), (1,)), ((), ())), preferred_element_type=f32
        )

    def multiply_early():
        normalize()
        for step in range(4):
            from_partner(step)

        @pl.loop(0, 14)
        def _(k):
            multiply(2 * ((z + 5 + k // 2) % Z) + k % 2)

    events = link_events()
    last_early = max(at for at, *what in events if what[-1] < 4)
    todo = []
    for at, kind, *what in events:
        act = functools.partial(on_sum if kind == "sum" else on_block, *what)
        todo.append((at, act))
        if kind == "sum" and what[-1] == 4:
            todo += [(at + 4.5, add_x), (max(at + 13.0, last_early + 0.1), multiply_early)]
    for _, act in sorted(todo, key=lambda item: item[0]):
        act()

    from_partner(4)
    for k in range(2):
        multiply(2 * turn_z(4) + k)

    quarter = t % 4
    for i in range(4):
        sent[i, :, 0:QCOLS] = acc_q[4 * i : 4 * i + 4, :].astype(bf16)
        sent[i, :, QCOLS:MSG] = acc_kv[4 * i : 4 * i + 4, :].astype(bf16)
    mixed[quarter] = sent[quarter]
    for d in range(1, 4):
        to = (quarter + d) % 4
        send(sent.at[to], mixed.at[quarter], e7_s.at[d], e7_r.at[d], dev(r, t - quarter + to))
    for g in range(GROUPS):
        pair[0:32, g * ROWS : (g + 1) * ROWS] = blocks[g, ROWS:BLOCK, 0:HEAD]
        pair[32:64, g * ROWS : (g + 1) * ROWS] = blocks[g, ROWS:BLOCK, HEAD:QCOLS]
    for copy in started[:-3]:
        copy.wait_send()
    for d in range(1, 4):
        frm = (quarter - d + 4) % 4
        arrived(mixed.at[frm], e7_r.at[d], dev(r, t - quarter + frm))
    for copy in started[-3:]:
        copy.wait_send()


def handoff(ids, gain, table, query, pairs):
    bf16, f32 = jnp.bfloat16, jnp.float32
    vmem = pl.BlockSpec(memory_space=pltpu.VMEM)
    hbm = pl.BlockSpec(memory_space=pltpu.HBM)
    dma = pltpu.SemaphoreType.DMA
    return pl.pallas_call(
        handoff_kernel,
        out_shape=(
            jax.ShapeDtypeStruct((GROUPS, BLOCK, QCOLS), bf16),
            jax.ShapeDtypeStruct((KVCOLS, GROUPS * ROWS), bf16),
            jax.ShapeDtypeStruct((4, 4, MSG), bf16),
        ),
        in_specs=[vmem, vmem, hbm, hbm, hbm],
        out_specs=(vmem, vmem, vmem),
        scratch_shapes=[
            pltpu.VMEM(table.shape, bf16),
            pltpu.VMEM(query.shape, bf16),
            pltpu.VMEM(pairs.shape, bf16),
            pltpu.VMEM((CORES, Z, XH, BATCH, FEAT), bf16),
            pltpu.VMEM((Z, XH, BATCH, FEAT), bf16),
            pltpu.VMEM((Z, XH, BATCH, FEAT), bf16),
            pltpu.VMEM((4, XH, BATCH, FEAT), bf16),
            pltpu.VMEM((4, XH, BATCH, FEAT), bf16),
            pltpu.VMEM((3, BATCH, FEAT), bf16),
            pltpu.VMEM((XH, BATCH, FEAT), bf16),
            pltpu.VMEM((TPS, 8, 2, 128), bf16),
            pltpu.VMEM((128, 256), f32),
            pltpu.VMEM((TPS, BATCH, FEAT), bf16),
            pltpu.VMEM((TPS, BATCH, FEAT), bf16),
            pltpu.VMEM((4, 4, MSG), bf16),
            pltpu.VMEM((BATCH, QCOLS), f32),
            pltpu.VMEM((BATCH, HEAD), f32),
            dma((3,)), dma((16,)), dma((16,)), dma((16,)), dma((16,)), dma((4, 2)), dma((4, 2)),
            dma((4, 2, 4)), dma((4, 2, 4)), dma((4, 2, 4)), dma((4, 2, 4)),
            dma((4, 9)), dma((4, 9)), dma((8,)), dma((8,)), dma((4,)), dma((4,)), dma((4,)), dma((4,)),
            dma((4,)), dma((4,)), dma((16,)), dma((16,)), dma((4,)), dma((4,)),
        ],
        compiler_params=pltpu.CompilerParams(
            collective_id=0, has_side_effects=True, vmem_limit_bytes=40 << 20
        ),
        cost_estimate=pl.CostEstimate(flops=1 << 34, bytes_accessed=1 << 23, transcendentals=0),
        name="handoff",
    )(ids, gain, table, query, pairs)


def attend_kernel(
    lengths, mixed, blocks, pair, keys_hbm, values_hbm, context, query_out, pair_out, keys, values, sems
):
    copies = [
        pltpu.make_async_copy(keys_hbm, keys, sems.at[0]),
        pltpu.make_async_copy(values_hbm, values, sems.at[1]),
        pltpu.make_async_copy(blocks.at[:, 0:ROWS, :], query_out, sems.at[2]),
        pltpu.make_async_copy(pair, pair_out, sems.at[3]),
    ]
    for copy in copies:
        copy.start()

    first = (lax.axis_index("tp") % 4) * 4
    got = [mixed[j].astype(jnp.float32) for j in range(4)]
    scale = HEAD ** (-0.5)
    copies[0].wait()
    rows = []
    for r in range(4):
        heads = [got[j][r : r + 1, k * HEAD : (k + 1) * HEAD] for j in range(4) for k in range(2)]
        query32 = jnp.concatenate(heads, axis=0)
        query = query32.astype(jnp.bfloat16)
        key_new = jnp.concatenate([got[j][r : r + 1, QCOLS : QCOLS + 32] for j in range(4)], axis=1)
        value_new = jnp.concatenate(
            [got[j][r : r + 1, QCOLS + 32 : QCOLS + 64] for j in range(4)], axis=1
        )
        scores = (
            lax.dot_general(
                query, keys[r], (((1,), (1,)), ((), ())), preferred_element_type=jnp.float32
            )
            * scale
        )
        position = lax.broadcasted_iota(jnp.int32, scores.shape, 1)
        scores = jnp.where(position < lengths[first + r], scores, -jnp.inf)
        own = jnp.sum(query32 * key_new, axis=1, keepdims=True) * scale
        top = jnp.maximum(jnp.max(scores, axis=1, keepdims=True), own)
        weights = jnp.exp(scores - top)
        own_weight = jnp.exp(own - top)
        total = jnp.sum(weights, axis=1, keepdims=True) + own_weight
        weights = (weights / total).astype(jnp.bfloat16)
        own_weight = (own_weight / total).astype(jnp.bfloat16).astype(jnp.float32)
        if r == 0:
            copies[1].wait()
        found = jnp.dot(weights, values[r], preferred_element_type=jnp.float32)
        rows.append(found + own_weight * value_new)
    lanes = [jnp.concatenate([rows[r][h : h + 1] for r in range(4)], axis=0) for h in range(GROUP)]
    context[...] = jnp.concatenate(lanes, axis=1).astype(jnp.bfloat16)
    copies[2].wait()
    copies[3].wait()


def attend(lengths, mixed, blocks, pair, keys, values):
    bf16 = jnp.bfloat16
    vmem = pl.BlockSpec(memory_space=pltpu.VMEM)
    anywhere = pl.BlockSpec(memory_space=pl.ANY)
    hbm = pl.BlockSpec(memory_space=pltpu.HBM)
    return pl.pallas_call(
        attend_kernel,
        out_shape=(
            jax.ShapeDtypeStruct((4, GROUP * HEAD), bf16),
            jax.ShapeDtypeStruct((GROUPS, ROWS, QCOLS), bf16),
            jax.ShapeDtypeStruct((KVCOLS, GROUPS * ROWS), bf16),
        ),
        in_specs=[pl.BlockSpec(memory_space=pltpu.SMEM), vmem, vmem, vmem, anywhere, anywhere],
        out_specs=(vmem, hbm, hbm),
        scratch_shapes=[
            pltpu.VMEM((4, 1024, HEAD), bf16),
            pltpu.VMEM((4, 1024, HEAD), bf16),
            pltpu.SemaphoreType.DMA((4,)),
        ],
        compiler_params=pltpu.CompilerParams(vmem_limit_bytes=24 << 20),
        name="attend",
    )(lengths, mixed, blocks, pair, keys, values)


def per_device(
    token_ids, embed_table, norm_gain, w_query, w_keyvalue, key_cache, value_cache, cache_lengths
):
    blocks, pair, mixed = handoff(
        token_ids.reshape(Z, XH * CORES * BATCH),
        norm_gain.reshape(TPS, 1, FEAT),
        *(pltpu.with_memory_space_constraint(a, pltpu.HBM) for a in (embed_table, w_query, w_keyvalue)),
    )
    context, query_full, pair_full = attend(cache_lengths, mixed, blocks, pair, key_cache, value_cache)
    return (
        context,
        query_full.reshape(GROUPS * ROWS, QCOLS),
        pair_full.reshape(2, 32, GROUPS * ROWS).transpose(2, 0, 1),
    )


def solution(mesh):
    both = ("replica", "tp")
    placed = (
        P(),
        P("replica", "tp"),
        P(),
        P(both, None),
        P(both, None, None),
        P(both, None, None),
        P(both, None, None),
        P("replica"),
    )
    return jax.shard_map(
        per_device,
        mesh=mesh,
        in_specs=placed,
        out_specs=(P(both, None), P(None, "tp"), P(None, None, "tp")),
        check_vma=False,
    )
```

```python
import functools
import math
import jax
import jax.numpy as jnp
from jax import lax
from jax.experimental import pallas as pl
from jax.experimental.pallas import tpu as pltpu
from jax.sharding import PartitionSpec as P

MESH = pl.DeviceIdType.MESH
Z, XH, CORES, TPS = 8, 4, 2, 16
GROUPS = Z * XH * CORES
BATCH, HEAD, GROUP, KVH = 16, 128, 8, 4
FEAT = 512
ROWS = 128
BLOCK = 320
SLOTS = 62
QCOLS = 256
KVCOLS = 64
MSG = 384


def link_events():
    lag = 2.2
    waiting, free, events = [(1.5, "sum", 0), (6.5, "own")], {"z": 0.0, "x": 0.0}, []

    def push(link, at, took, *what):
        free[link] = max(free[link], at) + took
        waiting.append((free[link] + lag, *what))

    while waiting:
        waiting.sort(key=lambda item: item[0])
        at, kind, *what = waiting.pop(0)
        events.append((at, kind, *what))
        step = what[0] if what else 0
        if kind == "sum":
            if step < 4:
                push("z", at, 1.4 if step else 0.7, "sum", step + 1)
            else:
                push("x", at, 1.4, "x_sum")
        elif kind == "own":
            push("z", at, 0.7, "z_first", 1)
            push("x", at, 2.1, "x_first", 1)
            push("z", at, 1.06, "ring", 1, 0)
            push("x", at, 1.4, "x_last", 1, 0)
        elif kind == "z_first":
            if step < 4:
                push("z", at, 0.7 if step < 3 else 0.35, "z_first", step + 1)
            push("x", at, 2.8 if step < 4 else 1.4, "x_last", 1, step)
        elif kind == "x_first":
            if step == 1:
                push("x", at, 1.05, "x_first", 2)
            for j in (1, 3) if step == 1 else (2,):
                push("z", at, 1.06, "ring", 1, j)
        elif kind == "ring" and step < 4:
            push("z", at, 1.06 if step < 3 else 0.53, "ring", step + 1, what[1])
        elif kind == "x_last" and step == 1:
            push("x", at, 1.4 if 0 < what[1] < 4 else 0.7, "x_last", 2, what[1])
    return events


def handoff_kernel(
    ids_hbm, gain_hbm, table_hbm, query_hbm, pair_hbm, blocks, pair, mixed,
    ids, gain, table, query, pairs, part, got_core, sums, up_sums, down_sums, got_x, sum_x, own_query, own_pairs, turned, embedded,
    normed, sent, acc_q, acc_kv,
    in_s, sems,
):
    r, t = lax.axis_index("replica"), lax.axis_index("tp")
    z, xh, c = r // 8, (r // 2) % 4, r % 2
    f32, bf16 = jnp.float32, jnp.bfloat16

    def rep(z_, xh_, c_):
        return (z_ * XH + xh_) * CORES + c_

    def dev(rep_, tp_):
        return {"replica": rep_, "tp": tp_}

    partner = dev(rep(z, xh, 1 - c), t)

    def x_peer(d):
        return dev(rep(z, (xh + d) % XH, c), t)

    def z_peer(d):
        return dev(rep((z + d) % Z, xh, c), t)

    def t_peer(d):
        return dev(r, (t + d) % TPS)

    loads = [
        pltpu.make_async_copy(table_hbm, table, in_s.at[0]),
        pltpu.make_async_copy(ids_hbm, ids, in_s.at[3]),
        pltpu.make_async_copy(gain_hbm, gain, in_s.at[4]),
        pltpu.make_async_copy(query_hbm, query, in_s.at[1]),
        pltpu.make_async_copy(pair_hbm, pairs, in_s.at[2]),
    ]
    for load in loads:
        load.start()
    barrier = pltpu.get_barrier_semaphore()
    peers = [partner] + [x_peer(d) for d in (1, 2, 3)] + [z_peer(1), z_peer(Z - 1)]
    peers += [t_peer(d) for d in range(1, 16)]
    for p in peers:
        pl.semaphore_signal(barrier, inc=1, device_id=p, device_id_type=MESH)

    slots, sent_rows = {}, {}

    def slot(*name):
        return sems.at[slots.setdefault(name, len(slots))]

    def send(src, dst, to, *name):
        kind = name[0]
        sent_rows[kind] = sent_rows.get(kind, 0) + math.prod(src.shape) // 128
        pltpu.make_async_remote_copy(
            src_ref=src, dst_ref=dst, send_sem=slot("sent", kind), recv_sem=slot(*name),
            device_id=to, device_id_type=MESH,
        ).start()

    def of_rows(rows, sem):
        for high in range(BLOCK, 0, -8):
            if rows == 36 or (rows % high == 0 and rows // high <= GROUPS):
                like = blocks.at[pl.ds(0, rows // high), pl.ds(0, high)]
                like = mixed.at[pl.ds(0, 3)] if rows == 36 else like
                return pltpu.make_async_remote_copy(
                    src_ref=like, dst_ref=like, send_sem=sem, recv_sem=sem,
                    device_id=partner, device_id_type=MESH,
                )
        raise ValueError(rows)

    def arrived(rows, *name):
        of_rows(rows, slot(*name)).wait_recv()

    base = r * table.shape[0]
    loads[0].wait()
    loads[1].wait()
    loads[2].wait()
    lane = lax.broadcasted_iota(jnp.int32, (128, 128), 1)

    @pl.loop(0, Z)
    def _(k):
        named = jnp.broadcast_to((ids[pl.ds(k, 1), :] - base).astype(f32), (128, 128)).T
        hot = jnp.concatenate(
            [(named == (lane + 128 * q).astype(f32)).astype(bf16) for q in range(8)], axis=1
        )
        rows = jnp.dot(hot, table[...], preferred_element_type=f32).astype(bf16)
        rows = rows.reshape(XH, CORES, BATCH, FEAT)
        part[0, k] = rows[:, 0]
        part[1, k] = rows[:, 1]

    own = rep(z, xh, c)
    heads_at = pl.multiple_of((t // 4) * 128, 128)
    loads[3].wait()
    loads[4].wait()
    own_query[t] = query[:, pl.ds(pl.multiple_of(t * QCOLS, QCOLS), QCOLS)]
    own_pairs[t] = pairs[:, :, pl.ds(heads_at, 128)]
    pl.semaphore_wait(barrier, len(peers))

    def turn_z(d):
        return (z + d) % Z

    far_first = (12, 4, 11, 5, 13, 3, 10, 6, 14, 2, 9, 7, 15, 1, 8)
    for d in (4, 3, 5, 2, 6, 1, 7, 0):
        at = turn_z(d)
        send(part.at[1 - c, at], got_core.at[at], partner, "core", d == 4)
    for d in far_first:
        to = (t + d) % TPS
        columns_of = pl.ds(pl.multiple_of(to * QCOLS, QCOLS), QCOLS)
        heads_of = pl.ds(pl.multiple_of((to // 4) * 128, 128), 128)
        send(query.at[:, columns_of], own_query.at[t], t_peer(d), "own_query")
        send(pairs.at[:, :, heads_of], own_pairs.at[t], t_peer(d), "own_pairs")

    def add_core(d):
        sums[turn_z(d)] = part[c, turn_z(d)] + got_core[turn_z(d)]

    def on_sum(step):
        up_dst, down_dst = up_sums.at[step], down_sums.at[step]
        if step == 0:
            arrived(256, "core", True)
            add_core(4)
            up, down = sums.at[turn_z(4), pl.ds(0, 2)], sums.at[turn_z(4), pl.ds(2, 2)]
            up_dst, down_dst = up_dst.at[pl.ds(0, 2)], down_dst.at[pl.ds(2, 2)]
        else:
            up, down = up_sums.at[step - 1], down_sums.at[step - 1]
            arrived(256 if step == 1 else 512, "sum", step)
            if step == 4:
                add_z()
                return
            above, below = turn_z(4 - step), turn_z(4 + step)
            if step == 1:
                up_sums[0, 0:2] = up_sums[0, 0:2] + sums[above, 0:2]
                up_sums[0, 2:4] = sums[above, 2:4]
                down_sums[0, 2:4] = down_sums[0, 2:4] + sums[below, 2:4]
                down_sums[0, 0:2] = sums[below, 0:2]
            else:
                up_sums[step - 1] = up_sums[step - 1] + sums[above]
                down_sums[step - 1] = down_sums[step - 1] + sums[below]
        send(up, up_dst, z_peer(1), "sum", step + 1)
        send(down, down_dst, z_peer(Z - 1), "sum", step + 1)
        if step == 0:
            arrived(7 * 256, "core", False)
            for d in (3, 5, 2, 6, 1, 7, 0):
                add_core(d)

    def add_z():
        sum_x[...] = (sums[z] + up_sums[3]) + down_sums[3]
        for d in (2, 1, 3):
            send(sum_x.at[(xh + d) % XH], got_x.at[d - 1], x_peer(d), "x_sum")

    def add_x():
        arrived(3 * 64, "x_sum")
        embedded[t] = (sum_x[xh] + got_x[0]) + (got_x[1] + got_x[2])
        for d in far_first:
            send(embedded.at[t], embedded.at[t], t_peer(d), "embedded")

    def whole_block():
        arrived(15 * 16, "own_pairs")
        even = lax.broadcasted_iota(jnp.int32, (256, 256), 1)
        even = jnp.where(even < 128, 2 * even, 2 * even - 255)
        pick = (lax.broadcasted_iota(jnp.int32, (256, 256), 0) == even).astype(bf16)
        turned[...] = lax.dot_general(
            own_pairs[...].reshape(256, 128), pick, (((0,), (0,)), ((), ())),
            preferred_element_type=f32,
        )
        mine = pl.multiple_of((t % 4) * 32, 32)
        blocks[own, 256:288, :] = turned[pl.ds(mine, 32), 0:128].astype(bf16)
        blocks[own, 288:320, :] = turned[pl.ds(mine, 32), 128:256].astype(bf16)
        arrived(15 * 16, "own_query")
        blocks[own, 128:256, :] = own_query[:, :, 128:256].reshape(ROWS, 128)
        blocks[own, 0:128, :] = own_query[:, :, 0:128].reshape(ROWS, 128)

    def group_at(dz, j, core):
        return rep((z + dz + 2 * Z) % Z, (xh - j + XH) % XH, core)

    def first_part(dz, j, core=c):
        return blocks.at[group_at(dz, j, core), pl.ds(0, 128)]

    def second_part(dz, j, core=c):
        return blocks.at[group_at(dz, j, core), pl.ds(128, 192)]

    def halved(ref, k):
        size = ref.shape[0] // 2
        return ref.at[pl.ds(k * size, size)]

    def column(j):
        return columns.at[:, (xh - j + XH) % XH, c, pl.ds(0, 128)]

    columns = blocks.reshape(Z, XH, CORES, BLOCK, 128)

    def column_to_partner(j):
        send(column(j), column(j), partner, "column")

    def to_partner(ref, step):
        send(ref, ref, partner, "mirrored", step)

    def z_first_on(step):
        up, down = first_part(-step, 0), first_part(step, 0)
        if step == 3:
            up, down = halved(up, 0), halved(down, 1)
        send(up, up, z_peer(1), "z_first", step + 1)
        send(down, down, z_peer(Z - 1), "z_first", step + 1)

    def offsets(step):
        return (step, -step) if 0 < step < 4 else (step,)

    def x_last_on(step):
        for dz in offsets(step):
            ref = first_part(dz, 0)
            send(ref, ref, x_peer(1), "x_last", 1, step)
            send(ref, ref, x_peer(3), "x_last", 1, step)

    def on_z_first(step):
        arrived(128 if step == 4 else 256, "z_first", step)
        if step < 4:
            z_first_on(step)
        x_last_on(step)
        if step == 4:
            column_to_partner(0)

    def on_x_last(hop, step):
        arrived(len(offsets(step)) * 256 // hop, "x_last", hop, step)
        if hop == 1:
            for dz in offsets(step):
                left, right = halved(first_part(dz, 1), 0), halved(first_part(dz, 3), 1)
                send(left, left, x_peer(1), "x_last", 2, step)
                send(right, right, x_peer(3), "x_last", 2, step)
        if step == 4:
            for j in (1, 3) if hop == 1 else (2,):
                column_to_partner(j)

    def to_ring(j, step):
        up, down = second_part(-step, j), second_part(step, j)
        if step == 3:
            up, down = halved(up, 0), halved(down, 1)
        send(up, up, z_peer(1), "ring", step + 1, j)
        send(down, down, z_peer(Z - 1), "ring", step + 1, j)

    def on_own():
        whole_block()
        z_first_on(0)
        ref = second_part(0, 0)
        send(ref, ref, x_peer(1), "x_first", 1)
        send(ref, ref, x_peer(3), "x_first", 1)
        to_ring(0, 0)
        x_last_on(0)
        to_partner(ref, 0)

    def on_x_first(hop):
        arrived(384 // hop, "x_first", hop)
        if hop == 1:
            left, right = halved(second_part(0, 1), 0), halved(second_part(0, 3), 1)
            send(left, left, x_peer(1), "x_first", 2)
            send(right, right, x_peer(3), "x_first", 2)
        for j in (1, 3) if hop == 1 else (2,):
            to_ring(j, 0)
            to_partner(second_part(0, j), 0)

    def on_ring(step, j):
        arrived(192 if step == 4 else 384, "ring", step, j)
        if step < 4:
            to_ring(j, step)
        up, down = second_part(-step, j), second_part(step, j)
        if step == 4:
            up, down = halved(up, 0), halved(down, 1)
        to_partner(up, step)
        to_partner(down, step)

    def from_partner(step):
        arrived(1536 if 0 < step < 4 else 768, "mirrored", step)

    def normalize():
        arrived(15 * 64, "embedded")

        def squares(k, total):
            v = embedded[k].astype(f32)
            return total + v * v

        squared = lax.fori_loop(0, TPS, squares, jnp.zeros((BATCH, FEAT), f32))
        mean_square = jnp.sum(squared, axis=1, keepdims=True) * (1.0 / (TPS * FEAT))
        factor = lax.rsqrt(mean_square + 1e-05)

        @pl.loop(0, TPS)
        def _(k):
            at_k = gain[pl.ds(pl.multiple_of(k * FEAT, FEAT), FEAT)]
            normed[k] = (embedded[k].astype(f32) * factor * at_k.astype(f32).reshape(1, FEAT)).astype(bf16)

    def matching(zz):
        return jnp.concatenate([normed[2 * zz], normed[2 * zz + 1]], axis=1)

    def multiply_second(offsets_z):
        q, kv = jnp.zeros((BATCH, 128), f32), jnp.zeros((BATCH, KVCOLS), f32)
        for zz in (turn_z(d) for d in offsets_z):
            lhs = matching(zz)
            rows = [blocks[8 * zz + i, 128:256, :] for i in range(8)]
            q += jnp.dot(lhs, jnp.concatenate(rows, axis=0), preferred_element_type=f32)
            both = jnp.concatenate([blocks[8 * zz + i, 256:320, :] for i in range(8)], axis=1)
            kv += lax.dot_general(
                lhs, both, (((1,), (1,)), ((), ())), preferred_element_type=f32
            )
        return q, kv

    def multiply_first(offsets_z):
        q = jnp.zeros((BATCH, 128), f32)
        for zz in (turn_z(d) for d in offsets_z):
            rows = [blocks[8 * zz + i, 0:128, :] for i in range(8)]
            q += jnp.dot(matching(zz), jnp.concatenate(rows, axis=0), preferred_element_type=f32)
        return q

    def multiply_early():
        normalize()
        for step in range(4):
            from_partner(step)
        acc_q[:, 128:256], acc_kv[:, 0:KVCOLS] = multiply_second((0, 1, 7, 2, 6, 3, 5))

    kinds = {
        "sum": on_sum, "own": on_own, "z_first": on_z_first, "x_first": on_x_first, "ring": on_ring,
        "x_last": on_x_last, "x_sum": add_x,
    }
    events = link_events()
    def order(kind, what):
        late = [("ring", 3, 2), ("x_last", 1, 4), ("early",), ("x_last", 2, 3), ("x_last", 2, 4), ("ring", 4, 2)]
        return late.index((kind, *what)) if (kind, *what) in late else -1

    todo = [(order(kind, what), at, functools.partial(kinds[kind], *what)) for at, kind, *what in events]
    todo.append((order("early", ()), 0.0, multiply_early))
    for *_, act in sorted(todo, key=lambda item: item[:2]):
        act()

    arrived(4096, "column")
    acc_q[:, 0:128] = multiply_first(range(Z))
    from_partner(4)
    q, kv = multiply_second((4,))
    acc_q[:, 128:256] += q
    acc_kv[:, 0:KVCOLS] += kv

    acc_kv[:, KVCOLS:128] = jnp.zeros((BATCH, 128 - KVCOLS), f32)
    quarter = t % 4
    for i in range(4):
        sent[i, :, 0:QCOLS] = acc_q[4 * i : 4 * i + 4, :].astype(bf16)
        sent[i, :, QCOLS:MSG] = acc_kv[4 * i : 4 * i + 4, :].astype(bf16)
    mixed[quarter] = sent[quarter]
    for d in range(1, 4):
        to = (quarter + d) % 4
        send(sent.at[to], mixed.at[quarter], dev(r, t - quarter + to), "mixed")
    for g in range(GROUPS):
        pair[:, g * ROWS : (g + 1) * ROWS] = blocks[g, 256:320, :]
    for kind, rows in sent_rows.items():
        if kind != "mixed":
            of_rows(rows, slot("sent", kind)).wait_send()
    arrived(sent_rows["mixed"], "mixed")
    of_rows(sent_rows["mixed"], slot("sent", "mixed")).wait_send()
    assert len(slots) == SLOTS, len(slots)


def handoff(ids, gain, table, query, pairs):
    bf16, f32 = jnp.bfloat16, jnp.float32
    vmem = pl.BlockSpec(memory_space=pltpu.VMEM)
    hbm = pl.BlockSpec(memory_space=pltpu.HBM)
    dma = pltpu.SemaphoreType.DMA
    return pl.pallas_call(
        handoff_kernel,
        out_shape=(
            jax.ShapeDtypeStruct((GROUPS, BLOCK, 128), bf16),
            jax.ShapeDtypeStruct((KVCOLS, GROUPS * ROWS), bf16),
            jax.ShapeDtypeStruct((4, 4, MSG), bf16),
        ),
        in_specs=[hbm] * 5,
        out_specs=(vmem, vmem, vmem),
        scratch_shapes=[
            pltpu.VMEM(ids.shape, jnp.int32),
            pltpu.VMEM(gain.shape, bf16),
            pltpu.VMEM(table.shape, bf16),
            pltpu.VMEM(query.shape, bf16),
            pltpu.VMEM(pairs.shape, bf16),
            pltpu.VMEM((CORES, Z, XH, BATCH, FEAT), bf16),
            pltpu.VMEM((Z, XH, BATCH, FEAT), bf16),
            pltpu.VMEM((Z, XH, BATCH, FEAT), bf16),
            pltpu.VMEM((4, XH, BATCH, FEAT), bf16),
            pltpu.VMEM((4, XH, BATCH, FEAT), bf16),
            pltpu.VMEM((3, BATCH, FEAT), bf16),
            pltpu.VMEM((XH, BATCH, FEAT), bf16),
            pltpu.VMEM((TPS, 8, QCOLS), bf16),
            pltpu.VMEM((TPS, 8, 2, 128), bf16),
            pltpu.VMEM((128, 256), f32),
            pltpu.VMEM((TPS, BATCH, FEAT), bf16),
            pltpu.VMEM((TPS, BATCH, FEAT), bf16),
            pltpu.VMEM((4, 4, MSG), bf16),
            pltpu.VMEM((BATCH, QCOLS), f32),
            pltpu.VMEM((BATCH, HEAD), f32),
            dma((5,)), dma((SLOTS,)),
        ],
        compiler_params=pltpu.CompilerParams(
            collective_id=0, has_side_effects=True, vmem_limit_bytes=40 << 20
        ),
        cost_estimate=pl.CostEstimate(flops=1 << 34, bytes_accessed=1 << 23, transcendentals=0),
        name="handoff",
    )(ids, gain, table, query, pairs)


def attend_kernel(
    lengths, mixed, blocks, pair, keys, values, context, query_out, pair_out, sems
):
    copies = [
        pltpu.make_async_copy(blocks.at[:, 0:128], query_out.at[:, :, 0:128], sems.at[0]),
        pltpu.make_async_copy(blocks.at[:, 128:256], query_out.at[:, :, 128:256], sems.at[1]),
        pltpu.make_async_copy(pair, pair_out, sems.at[2]),
    ]
    for copy in copies:
        copy.start()

    first = (lax.axis_index("tp") % 4) * 4
    got = [mixed[j].astype(jnp.float32) for j in range(4)]
    scale = HEAD ** (-0.5)
    queries, own, scores, lens, new_values = [], [], [], [], []
    for r in range(4):
        heads = [got[j][r : r + 1, k * HEAD : (k + 1) * HEAD] for j in range(4) for k in range(2)]
        query32 = jnp.concatenate(heads, axis=0)
        query = query32.astype(jnp.bfloat16)
        key_new = jnp.concatenate([got[j][r : r + 1, QCOLS : QCOLS + 32] for j in range(4)], axis=1)
        new_values.append(
            jnp.concatenate([got[j][r : r + 1, QCOLS + 32 : QCOLS + 64] for j in range(4)], axis=1)
        )
        scores.append(
            lax.dot_general(
                query, keys[r], (((1,), (1,)), ((), ())), preferred_element_type=jnp.float32
            )
        )
        own.append(jnp.sum(query32 * key_new, axis=1, keepdims=True) * scale)
        lens.append(jnp.full((GROUP, 1), lengths[first + r], jnp.int32))
    scores = jnp.concatenate(scores, axis=0) * scale
    own, lens = jnp.concatenate(own, axis=0), jnp.concatenate(lens, axis=0)
    position = lax.broadcasted_iota(jnp.int32, scores.shape, 1)
    scores = jnp.where(position < lens, scores, -jnp.inf)
    top = jnp.maximum(jnp.max(scores, axis=1, keepdims=True), own)
    weights = jnp.exp(scores - top)
    own_weight = jnp.exp(own - top)
    total = jnp.sum(weights, axis=1, keepdims=True) + own_weight
    weights = (weights / total).astype(jnp.bfloat16)
    own_weight = (own_weight / total).astype(jnp.bfloat16).astype(jnp.float32)
    rows = []
    for r in range(4):
        mine = slice(r * GROUP, (r + 1) * GROUP)
        found = jnp.dot(weights[mine], values[r], preferred_element_type=jnp.float32)
        rows.append(found + own_weight[mine] * new_values[r])
    lanes = [jnp.concatenate([rows[r][h : h + 1] for r in range(4)], axis=0) for h in range(GROUP)]
    context[...] = jnp.concatenate(lanes, axis=1).astype(jnp.bfloat16)
    for copy in copies:
        copy.wait()


def attend(lengths, mixed, blocks, pair, keys, values):
    bf16 = jnp.bfloat16
    vmem = pl.BlockSpec(memory_space=pltpu.VMEM)
    hbm = pl.BlockSpec(memory_space=pltpu.HBM)
    return pl.pallas_call(
        attend_kernel,
        out_shape=(
            jax.ShapeDtypeStruct((4, GROUP * HEAD), bf16),
            jax.ShapeDtypeStruct((GROUPS, ROWS, QCOLS), bf16),
            jax.ShapeDtypeStruct((KVCOLS, GROUPS * ROWS), bf16),
        ),
        in_specs=[pl.BlockSpec(memory_space=pltpu.SMEM), vmem, vmem, vmem, vmem, vmem],
        out_specs=(vmem, hbm, hbm),
        scratch_shapes=[
            pltpu.SemaphoreType.DMA((3,)),
        ],
        compiler_params=pltpu.CompilerParams(vmem_limit_bytes=24 << 20),
        name="attend",
    )(lengths, mixed, blocks, pair, keys, values)


def per_device(
    token_ids, embed_table, norm_gain, w_query, w_keyvalue, key_cache, value_cache, cache_lengths
):
    blocks, pair, mixed = handoff(
        *(
            pltpu.with_memory_space_constraint(a, pltpu.HBM)
            for a in (
                token_ids.reshape(Z, XH * CORES * BATCH), norm_gain, embed_table, w_query, w_keyvalue
            )
        ),
    )
    context, query_full, pair_full = attend(cache_lengths, mixed, blocks, pair, key_cache, value_cache)
    return (
        context,
        query_full.reshape(GROUPS * ROWS, QCOLS),
        pair_full.reshape(2, 32, GROUPS * ROWS).transpose(2, 0, 1),
    )


def solution(mesh):
    both = ("replica", "tp")
    placed = (
        P(),
        P("replica", "tp"),
        P(),
        P(both, None),
        P(both, None, None),
        P(both, None, None),
        P(both, None, None),
        P("replica"),
    )
    return jax.shard_map(
        per_device,
        mesh=mesh,
        in_specs=placed,
        out_specs=(P(both, None), P(None, "tp"), P(None, None, "tp")),
        check_vma=False,
    )
```

```python
import functools
import math
import jax
import jax.numpy as jnp
from jax import lax
from jax.experimental import pallas as pl
from jax.experimental.pallas import tpu as pltpu
from jax.sharding import PartitionSpec as P

MESH = pl.DeviceIdType.MESH
Z, XH, CORES, TPS = 8, 4, 2, 16
GROUPS = Z * XH * CORES
BATCH, HEAD, GROUP, KVH = 16, 128, 8, 4
FEAT = 512
ROWS = 128
BLOCK = 320
SLOTS = 62
QCOLS = 256
KVCOLS = 64
MSG = 384


def link_events():
    lag = {"z": 3.2, "x": 2.2}
    waiting, free, events = [(1.5, "sum", 0), (6.5, "own")], {"z": 0.0, "x": 0.0}, []

    def push(link, at, took, *what):
        free[link] = max(free[link], at) + took
        waiting.append((free[link] + lag[link], *what))

    while waiting:
        waiting.sort(key=lambda item: item[0])
        at, kind, *what = waiting.pop(0)
        events.append((at, kind, *what))
        step = what[0] if what else 0
        if kind == "sum":
            if step < 4:
                push("z", at, 1.4 if step else 0.7, "sum", step + 1)
            else:
                push("x", at, 1.4, "x_sum")
        elif kind == "own":
            push("z", at, 0.7, "z_first", 1)
            push("x", at, 2.1, "x_first", 1)
            push("z", at, 1.06, "ring", 1, 0)
            push("x", at, 1.4, "x_last", 1, 0)
        elif kind == "z_first":
            if step < 4:
                push("z", at, 0.7 if step < 3 else 0.35, "z_first", step + 1)
            push("x", at, 2.8 if step < 4 else 1.4, "x_last", 1, step)
        elif kind == "x_first":
            if step == 1:
                push("x", at, 1.05, "x_first", 2)
            for j in (1, 3) if step == 1 else (2,):
                push("z", at, 1.06, "ring", 1, j)
        elif kind == "ring" and step < 4:
            push("z", at, 1.06 if step < 3 else 0.53, "ring", step + 1, what[1])
        elif kind == "x_last" and step == 1:
            push("x", at, 1.4 if 0 < what[1] < 4 else 0.7, "x_last", 2, what[1])
    return events


def handoff_kernel(
    ids_hbm, gain_hbm, table_hbm, query_hbm, pair_hbm, blocks, pair, mixed,
    ids, gain, table, query, pairs, part, got_core, sums, up_sums, down_sums, got_x, sum_x, own_query, own_pairs, turned, embedded,
    normed, sent, acc_q, acc_kv,
    in_s, sems,
):
    r, t = lax.axis_index("replica"), lax.axis_index("tp")
    z, xh, c = r // 8, (r // 2) % 4, r % 2
    f32, bf16 = jnp.float32, jnp.bfloat16

    def rep(z_, xh_, c_):
        return (z_ * XH + xh_) * CORES + c_

    def dev(rep_, tp_):
        return {"replica": rep_, "tp": tp_}

    partner = dev(rep(z, xh, 1 - c), t)

    def x_peer(d):
        return dev(rep(z, (xh + d) % XH, c), t)

    def z_peer(d):
        return dev(rep((z + d) % Z, xh, c), t)

    def t_peer(d):
        return dev(r, (t + d) % TPS)

    loads = [
        pltpu.make_async_copy(table_hbm, table, in_s.at[0]),
        pltpu.make_async_copy(ids_hbm, ids, in_s.at[3]),
        pltpu.make_async_copy(gain_hbm, gain, in_s.at[4]),
        pltpu.make_async_copy(query_hbm, query, in_s.at[1]),
        pltpu.make_async_copy(pair_hbm, pairs, in_s.at[2]),
    ]
    for load in loads:
        load.start()
    barrier = pltpu.get_barrier_semaphore()
    peers = [partner] + [x_peer(d) for d in (1, 2, 3)] + [z_peer(1), z_peer(Z - 1)]
    peers += [t_peer(d) for d in range(1, 16)]
    for p in peers:
        pl.semaphore_signal(barrier, inc=1, device_id=p, device_id_type=MESH)

    slots, sent_rows = {}, {}

    def slot(*name):
        return sems.at[slots.setdefault(name, len(slots))]

    def send(src, dst, to, *name):
        kind = name[0]
        sent_rows[kind] = sent_rows.get(kind, 0) + math.prod(src.shape) // 128
        pltpu.make_async_remote_copy(
            src_ref=src, dst_ref=dst, send_sem=slot("sent", kind), recv_sem=slot(*name),
            device_id=to, device_id_type=MESH,
        ).start()

    def of_rows(rows, sem):
        for high in range(BLOCK, 0, -8):
            if rows == 36 or (rows % high == 0 and rows // high <= GROUPS):
                like = blocks.at[pl.ds(0, rows // high), pl.ds(0, high)]
                like = mixed.at[pl.ds(0, 3)] if rows == 36 else like
                return pltpu.make_async_remote_copy(
                    src_ref=like, dst_ref=like, send_sem=sem, recv_sem=sem,
                    device_id=partner, device_id_type=MESH,
                )
        raise ValueError(rows)

    def arrived(rows, *name):
        of_rows(rows, slot(*name)).wait_recv()

    base = r * table.shape[0]
    loads[0].wait()
    loads[1].wait()
    loads[2].wait()
    lane = lax.broadcasted_iota(jnp.int32, (128, 128), 1)

    @pl.loop(0, Z)
    def _(k):
        named = jnp.broadcast_to((ids[pl.ds(k, 1), :] - base).astype(f32), (128, 128)).T
        hot = jnp.concatenate(
            [(named == (lane + 128 * q).astype(f32)).astype(bf16) for q in range(8)], axis=1
        )
        rows = jnp.dot(hot, table[...], preferred_element_type=f32).astype(bf16)
        rows = rows.reshape(XH, CORES, BATCH, FEAT)
        part[0, k] = rows[:, 0]
        part[1, k] = rows[:, 1]

    own = rep(z, xh, c)
    heads_at = pl.multiple_of((t // 4) * 128, 128)
    loads[3].wait()
    loads[4].wait()
    own_query[t] = query[:, pl.ds(pl.multiple_of(t * QCOLS, QCOLS), QCOLS)]
    own_pairs[t] = pairs[:, :, pl.ds(heads_at, 128)]
    pl.semaphore_wait(barrier, len(peers))

    def turn_z(d):
        return (z + d) % Z

    far_first = (12, 4, 11, 5, 13, 3, 10, 6, 14, 2, 9, 7, 15, 1, 8)
    for d in (4, 3, 5, 2, 6, 1, 7, 0):
        at = turn_z(d)
        send(part.at[1 - c, at], got_core.at[at], partner, "core", d == 4)
    for d in far_first:
        to = (t + d) % TPS
        columns_of = pl.ds(pl.multiple_of(to * QCOLS, QCOLS), QCOLS)
        heads_of = pl.ds(pl.multiple_of((to // 4) * 128, 128), 128)
        send(query.at[:, columns_of], own_query.at[t], t_peer(d), "own_query")
        send(pairs.at[:, :, heads_of], own_pairs.at[t], t_peer(d), "own_pairs")

    def add_core(d):
        sums[turn_z(d)] = part[c, turn_z(d)] + got_core[turn_z(d)]

    def on_sum(step):
        up_dst, down_dst = up_sums.at[step], down_sums.at[step]
        if step == 0:
            arrived(256, "core", True)
            add_core(4)
            up, down = sums.at[turn_z(4), pl.ds(0, 2)], sums.at[turn_z(4), pl.ds(2, 2)]
            up_dst, down_dst = up_dst.at[pl.ds(0, 2)], down_dst.at[pl.ds(2, 2)]
        else:
            up, down = up_sums.at[step - 1], down_sums.at[step - 1]
            arrived(256 if step == 1 else 512, "sum", step)
            if step == 4:
                add_z()
                return
            above, below = turn_z(4 - step), turn_z(4 + step)
            if step == 1:
                up_sums[0, 0:2] = up_sums[0, 0:2] + sums[above, 0:2]
                up_sums[0, 2:4] = sums[above, 2:4]
                down_sums[0, 2:4] = down_sums[0, 2:4] + sums[below, 2:4]
                down_sums[0, 0:2] = sums[below, 0:2]
            else:
                up_sums[step - 1] = up_sums[step - 1] + sums[above]
                down_sums[step - 1] = down_sums[step - 1] + sums[below]
        send(up, up_dst, z_peer(1), "sum", step + 1)
        send(down, down_dst, z_peer(Z - 1), "sum", step + 1)
        if step == 0:
            arrived(7 * 256, "core", False)
            for d in (3, 5, 2, 6, 1, 7, 0):
                add_core(d)

    def add_z():
        sum_x[...] = (sums[z] + up_sums[3]) + down_sums[3]
        for d in (2, 1, 3):
            send(sum_x.at[(xh + d) % XH], got_x.at[d - 1], x_peer(d), "x_sum")

    def add_x():
        arrived(3 * 64, "x_sum")
        embedded[t] = (sum_x[xh] + got_x[0]) + (got_x[1] + got_x[2])
        for d in far_first:
            send(embedded.at[t], embedded.at[t], t_peer(d), "embedded")

    def whole_block():
        arrived(15 * 16, "own_pairs")
        even = lax.broadcasted_iota(jnp.int32, (256, 256), 1)
        even = jnp.where(even < 128, 2 * even, 2 * even - 255)
        pick = (lax.broadcasted_iota(jnp.int32, (256, 256), 0) == even).astype(bf16)
        turned[...] = lax.dot_general(
            own_pairs[...].reshape(256, 128), pick, (((0,), (0,)), ((), ())),
            preferred_element_type=f32,
        )
        mine = pl.multiple_of((t % 4) * 32, 32)
        blocks[own, 256:288, :] = turned[pl.ds(mine, 32), 0:128].astype(bf16)
        blocks[own, 288:320, :] = turned[pl.ds(mine, 32), 128:256].astype(bf16)
        arrived(15 * 16, "own_query")
        blocks[own, 128:256, :] = own_query[:, :, 128:256].reshape(ROWS, 128)
        blocks[own, 0:128, :] = own_query[:, :, 0:128].reshape(ROWS, 128)

    def group_at(dz, j, core):
        return rep((z + dz + 2 * Z) % Z, (xh - j + XH) % XH, core)

    def first_part(dz, j, core=c):
        return blocks.at[group_at(dz, j, core), pl.ds(0, 128)]

    def second_part(dz, j, core=c):
        return blocks.at[group_at(dz, j, core), pl.ds(128, 192)]

    def halved(ref, k):
        size = ref.shape[0] // 2
        return ref.at[pl.ds(k * size, size)]

    def column(j):
        return columns.at[:, (xh - j + XH) % XH, c, pl.ds(0, 128)]

    columns = blocks.reshape(Z, XH, CORES, BLOCK, 128)

    def column_to_partner(j):
        send(column(j), column(j), partner, "column")

    def to_partner(ref, step):
        send(ref, ref, partner, "mirrored", step)

    def z_first_on(step):
        up, down = first_part(-step, 0), first_part(step, 0)
        if step == 3:
            up, down = halved(up, 0), halved(down, 1)
        send(up, up, z_peer(1), "z_first", step + 1)
        send(down, down, z_peer(Z - 1), "z_first", step + 1)

    def offsets(step):
        return (step, -step) if 0 < step < 4 else (step,)

    def x_last_on(step):
        for dz in offsets(step):
            ref = first_part(dz, 0)
            send(ref, ref, x_peer(1), "x_last", 1, step)
            send(ref, ref, x_peer(3), "x_last", 1, step)

    def on_z_first(step):
        arrived(128 if step == 4 else 256, "z_first", step)
        if step < 4:
            z_first_on(step)
        x_last_on(step)
        if step == 4:
            column_to_partner(0)

    def on_x_last(hop, step):
        arrived(len(offsets(step)) * 256 // hop, "x_last", hop, step)
        if hop == 1:
            for dz in offsets(step):
                left, right = halved(first_part(dz, 1), 0), halved(first_part(dz, 3), 1)
                send(left, left, x_peer(1), "x_last", 2, step)
                send(right, right, x_peer(3), "x_last", 2, step)
        if step == 4:
            for j in (1, 3) if hop == 1 else (2,):
                column_to_partner(j)

    def to_ring(j, step):
        up, down = second_part(-step, j), second_part(step, j)
        if step == 3:
            up, down = halved(up, 0), halved(down, 1)
        send(up, up, z_peer(1), "ring", step + 1, j)
        send(down, down, z_peer(Z - 1), "ring", step + 1, j)

    def on_own():
        whole_block()
        z_first_on(0)
        ref = second_part(0, 0)
        send(ref, ref, x_peer(1), "x_first", 1)
        send(ref, ref, x_peer(3), "x_first", 1)
        to_ring(0, 0)
        x_last_on(0)
        to_partner(ref, 0)

    def on_x_first(hop):
        arrived(384 // hop, "x_first", hop)
        if hop == 1:
            left, right = halved(second_part(0, 1), 0), halved(second_part(0, 3), 1)
            send(left, left, x_peer(1), "x_first", 2)
            send(right, right, x_peer(3), "x_first", 2)
        for j in (1, 3) if hop == 1 else (2,):
            to_ring(j, 0)
            to_partner(second_part(0, j), 0)

    def on_ring(step, j):
        arrived(192 if step == 4 else 384, "ring", step, j)
        if step < 4:
            to_ring(j, step)
        up, down = second_part(-step, j), second_part(step, j)
        if step == 4:
            up, down = halved(up, 0), halved(down, 1)
        to_partner(up, step)
        to_partner(down, step)

    def from_partner(step):
        arrived(1536 if 0 < step < 4 else 768, "mirrored", step)

    def normalize():
        arrived(15 * 64, "embedded")

        def squares(k, total):
            v = embedded[k].astype(f32)
            return total + v * v

        squared = lax.fori_loop(0, TPS, squares, jnp.zeros((BATCH, FEAT), f32))
        mean_square = jnp.sum(squared, axis=1, keepdims=True) * (1.0 / (TPS * FEAT))
        factor = lax.rsqrt(mean_square + 1e-05)

        @pl.loop(0, TPS)
        def _(k):
            at_k = gain[pl.ds(pl.multiple_of(k * FEAT, FEAT), FEAT)]
            normed[k] = (embedded[k].astype(f32) * factor * at_k.astype(f32).reshape(1, FEAT)).astype(bf16)

    def matching(zz):
        return jnp.concatenate([normed[2 * zz], normed[2 * zz + 1]], axis=1)

    def multiply_second(offsets_z):
        q, kv = jnp.zeros((BATCH, 128), f32), jnp.zeros((BATCH, KVCOLS), f32)
        for zz in (turn_z(d) for d in offsets_z):
            lhs = matching(zz)
            rows = [blocks[8 * zz + i, 128:256, :] for i in range(8)]
            q += jnp.dot(lhs, jnp.concatenate(rows, axis=0), preferred_element_type=f32)
            both = jnp.concatenate([blocks[8 * zz + i, 256:320, :] for i in range(8)], axis=1)
            kv += lax.dot_general(
                lhs, both, (((1,), (1,)), ((), ())), preferred_element_type=f32
            )
        return q, kv

    def multiply_first(offsets_z):
        q = jnp.zeros((BATCH, 128), f32)
        for zz in (turn_z(d) for d in offsets_z):
            rows = [blocks[8 * zz + i, 0:128, :] for i in range(8)]
            q += jnp.dot(matching(zz), jnp.concatenate(rows, axis=0), preferred_element_type=f32)
        return q

    def multiply_early():
        normalize()
        for step in range(4):
            from_partner(step)
        acc_q[:, 128:256], acc_kv[:, 0:KVCOLS] = multiply_second((0, 1, 7, 2, 6, 3, 5))

    kinds = {
        "sum": on_sum, "own": on_own, "z_first": on_z_first, "x_first": on_x_first, "ring": on_ring,
        "x_last": on_x_last, "x_sum": add_x,
    }
    events = link_events()
    def order(kind, what):
        late = [("ring", 3, 2), ("x_last", 1, 4), ("early",), ("x_last", 2, 3), ("x_last", 2, 4), ("ring", 4, 2)]
        return late.index((kind, *what)) if (kind, *what) in late else -1

    todo = [(order(kind, what), at, functools.partial(kinds[kind], *what)) for at, kind, *what in events]
    todo.append((order("early", ()), 0.0, multiply_early))
    for *_, act in sorted(todo, key=lambda item: item[:2]):
        act()

    arrived(4096, "column")
    acc_q[:, 0:128] = multiply_first(range(Z))
    from_partner(4)
    q, kv = multiply_second((4,))
    acc_q[:, 128:256] += q
    acc_kv[:, 0:KVCOLS] += kv

    acc_kv[:, KVCOLS:128] = jnp.zeros((BATCH, 128 - KVCOLS), f32)
    quarter = t % 4
    for i in range(4):
        sent[i, :, 0:QCOLS] = acc_q[4 * i : 4 * i + 4, :].astype(bf16)
        sent[i, :, QCOLS:MSG] = acc_kv[4 * i : 4 * i + 4, :].astype(bf16)
    mixed[quarter] = sent[quarter]
    for d in range(1, 4):
        to = (quarter + d) % 4
        send(sent.at[to], mixed.at[quarter], dev(r, t - quarter + to), "mixed")
    for g in range(GROUPS):
        pair[:, g * ROWS : (g + 1) * ROWS] = blocks[g, 256:320, :]
    for kind, rows in sent_rows.items():
        if kind != "mixed":
            of_rows(rows, slot("sent", kind)).wait_send()
    arrived(sent_rows["mixed"], "mixed")
    of_rows(sent_rows["mixed"], slot("sent", "mixed")).wait_send()
    assert len(slots) == SLOTS, len(slots)


def handoff(ids, gain, table, query, pairs):
    bf16, f32 = jnp.bfloat16, jnp.float32
    vmem = pl.BlockSpec(memory_space=pltpu.VMEM)
    hbm = pl.BlockSpec(memory_space=pltpu.HBM)
    dma = pltpu.SemaphoreType.DMA
    return pl.pallas_call(
        handoff_kernel,
        out_shape=(
            jax.ShapeDtypeStruct((GROUPS, BLOCK, 128), bf16),
            jax.ShapeDtypeStruct((KVCOLS, GROUPS * ROWS), bf16),
            jax.ShapeDtypeStruct((4, 4, MSG), bf16),
        ),
        in_specs=[hbm] * 5,
        out_specs=(vmem, vmem, vmem),
        scratch_shapes=[
            pltpu.VMEM(ids.shape, jnp.int32),
            pltpu.VMEM(gain.shape, bf16),
            pltpu.VMEM(table.shape, bf16),
            pltpu.VMEM(query.shape, bf16),
            pltpu.VMEM(pairs.shape, bf16),
            pltpu.VMEM((CORES, Z, XH, BATCH, FEAT), bf16),
            pltpu.VMEM((Z, XH, BATCH, FEAT), bf16),
            pltpu.VMEM((Z, XH, BATCH, FEAT), bf16),
            pltpu.VMEM((4, XH, BATCH, FEAT), bf16),
            pltpu.VMEM((4, XH, BATCH, FEAT), bf16),
            pltpu.VMEM((3, BATCH, FEAT), bf16),
            pltpu.VMEM((XH, BATCH, FEAT), bf16),
            pltpu.VMEM((TPS, 8, QCOLS), bf16),
            pltpu.VMEM((TPS, 8, 2, 128), bf16),
            pltpu.VMEM((128, 256), f32),
            pltpu.VMEM((TPS, BATCH, FEAT), bf16),
            pltpu.VMEM((TPS, BATCH, FEAT), bf16),
            pltpu.VMEM((4, 4, MSG), bf16),
            pltpu.VMEM((BATCH, QCOLS), f32),
            pltpu.VMEM((BATCH, HEAD), f32),
            dma((5,)), dma((SLOTS,)),
        ],
        compiler_params=pltpu.CompilerParams(
            collective_id=0, has_side_effects=True, vmem_limit_bytes=40 << 20
        ),
        cost_estimate=pl.CostEstimate(flops=1 << 34, bytes_accessed=1 << 23, transcendentals=0),
        name="handoff",
    )(ids, gain, table, query, pairs)


def attend_kernel(
    lengths, mixed, blocks, pair, keys, values, context, query_out, pair_out, sems
):
    copies = [
        pltpu.make_async_copy(
            blocks.at[pl.ds(16 * k, 16), pl.ds(128 * half, 128)],
            query_out.at[pl.ds(16 * k, 16), :, pl.ds(128 * half, 128)],
            sems.at[2 * k + half],
        )
        for k in range(4)
        for half in range(2)
    ]
    copies += [
        pltpu.make_async_copy(
            pair.at[pl.ds(32 * k, 32)], pair_out.at[pl.ds(32 * k, 32)], sems.at[8 + k]
        )
        for k in range(2)
    ]
    for copy in copies:
        copy.start()

    first = (lax.axis_index("tp") % 4) * 4
    got = [mixed[j].astype(jnp.float32) for j in range(4)]
    scale = HEAD ** (-0.5)
    queries, own, scores, lens, new_values = [], [], [], [], []
    for r in range(4):
        heads = [got[j][r : r + 1, k * HEAD : (k + 1) * HEAD] for j in range(4) for k in range(2)]
        query32 = jnp.concatenate(heads, axis=0)
        query = query32.astype(jnp.bfloat16)
        key_new = jnp.concatenate([got[j][r : r + 1, QCOLS : QCOLS + 32] for j in range(4)], axis=1)
        new_values.append(
            jnp.concatenate([got[j][r : r + 1, QCOLS + 32 : QCOLS + 64] for j in range(4)], axis=1)
        )
        scores.append(
            lax.dot_general(
                query, keys[r], (((1,), (1,)), ((), ())), preferred_element_type=jnp.float32
            )
        )
        own.append(jnp.sum(query32 * key_new, axis=1, keepdims=True) * scale)
        lens.append(jnp.full((GROUP, 1), lengths[first + r], jnp.int32))
    scores = jnp.concatenate(scores, axis=0) * scale
    own, lens = jnp.concatenate(own, axis=0), jnp.concatenate(lens, axis=0)
    position = lax.broadcasted_iota(jnp.int32, scores.shape, 1)
    scores = jnp.where(position < lens, scores, -jnp.inf)
    top = jnp.maximum(jnp.max(scores, axis=1, keepdims=True), own)
    weights = jnp.exp(scores - top)
    own_weight = jnp.exp(own - top)
    total = jnp.sum(weights, axis=1, keepdims=True) + own_weight
    weights = (weights / total).astype(jnp.bfloat16)
    own_weight = (own_weight / total).astype(jnp.bfloat16).astype(jnp.float32)
    rows = []
    for r in range(4):
        mine = slice(r * GROUP, (r + 1) * GROUP)
        found = jnp.dot(weights[mine], values[r], preferred_element_type=jnp.float32)
        rows.append(found + own_weight[mine] * new_values[r])
    lanes = [jnp.concatenate([rows[r][h : h + 1] for r in range(4)], axis=0) for h in range(GROUP)]
    context[...] = jnp.concatenate(lanes, axis=1).astype(jnp.bfloat16)
    for copy in copies:
        copy.wait()


def attend(lengths, mixed, blocks, pair, keys, values):
    bf16 = jnp.bfloat16
    vmem = pl.BlockSpec(memory_space=pltpu.VMEM)
    hbm = pl.BlockSpec(memory_space=pltpu.HBM)
    return pl.pallas_call(
        attend_kernel,
        out_shape=(
            jax.ShapeDtypeStruct((4, GROUP * HEAD), bf16),
            jax.ShapeDtypeStruct((GROUPS, ROWS, QCOLS), bf16),
            jax.ShapeDtypeStruct((KVCOLS, GROUPS * ROWS), bf16),
        ),
        in_specs=[pl.BlockSpec(memory_space=pltpu.SMEM), vmem, vmem, vmem, vmem, vmem],
        out_specs=(vmem, hbm, hbm),
        scratch_shapes=[
            pltpu.SemaphoreType.DMA((10,)),
        ],
        compiler_params=pltpu.CompilerParams(vmem_limit_bytes=24 << 20),
        name="attend",
    )(lengths, mixed, blocks, pair, keys, values)


def per_device(
    token_ids, embed_table, norm_gain, w_query, w_keyvalue, key_cache, value_cache, cache_lengths
):
    blocks, pair, mixed = handoff(
        *(
            pltpu.with_memory_space_constraint(a, pltpu.HBM)
            for a in (
                token_ids.reshape(Z, XH * CORES * BATCH), norm_gain, embed_table, w_query, w_keyvalue
            )
        ),
    )
    context, query_full, pair_full = attend(cache_lengths, mixed, blocks, pair, key_cache, value_cache)
    return (
        context,
        query_full.reshape(GROUPS * ROWS, QCOLS),
        pair_full.reshape(2, 32, GROUPS * ROWS).transpose(2, 0, 1),
    )


def solution(mesh):
    both = ("replica", "tp")
    placed = (
        P(),
        P("replica", "tp"),
        P(),
        P(both, None),
        P(both, None, None),
        P(both, None, None),
        P(both, None, None),
        P("replica"),
    )
    return jax.shard_map(
        per_device,
        mesh=mesh,
        in_specs=placed,
        out_specs=(P(both, None), P(None, "tp"), P(None, None, "tp")),
        check_vma=False,
    )
```
